32 devices in a mesh: pages: 8 (over z, y), heads: 4 (over x, core).
Axes of the slice: x: 2, y: 2, z: 4, core: 2. Of those that a mesh axis runs over, the one named last changes fastest.
Arguments:
- x_in: bfloat16 [32, 561, 768], P('pages'), may hold values from -6 to 6
- cotangent: bfloat16 [32, 561, 768], P('pages'), may hold values from -6 to 6
- text_len: int32 [32], P('pages'), may hold values from 40 to 512, as said below
- coords: int32 [32, 3, 561], P('pages'), may hold values from 0 to 255
- grid_index: int32 [32, 49], P('pages'), may hold values from 0 to 48, each once within a row
- w_qkv: bfloat16 [768, 3, 768], P('pages', None, 'heads'), may hold values from -0.21875 to 0.21875
- b_qv: bfloat16 [2, 768], P(None, ('heads', 'pages')), may hold values from -3 to 3
- w_out: bfloat16 [768, 768], P(('heads', 'pages')), may hold values from -0.875 to 0.875
- w_up: bfloat16 [768, 3072], P('pages', 'heads'), may hold values from -0.21875 to 0.21875
- b_up: bfloat16 [3072], P(('heads', 'pages')), may hold values from -3 to 3
- w_down: bfloat16 [3072, 768], P(('heads', 'pages')), may hold values from -0.109375 to 0.109375
- rel_bias: bfloat16 [3, 128, 12], P(None, 'pages', 'heads'), may hold values from -3 to 3
- conv_w: bfloat16 [18, 768], P(None, ('pages', 'heads')), may hold values from -2 to 2
- biases: bfloat16 [6, 768], P(None, ('pages', 'heads')), may hold values from -2 to 2
- gains: bfloat16 [2, 768], P(None, ('pages', 'heads')), may hold values from 0.5 to 1.5
Outputs:
- out: bfloat16 [32, 561, 768], P('pages')
- grad_x: float32 [32, 561, 768], P('pages')
- grad_w_qkv: float32 [768, 3, 768], P('pages', None, 'heads')
- grad_b_qv: float32 [2, 768], P(None, ('heads', 'pages'))
- grad_w_out: float32 [768, 768], P(('heads', 'pages'))
- grad_w_up: float32 [768, 3072], P('pages', 'heads')
- grad_b_up: float32 [3072], P(('heads', 'pages'))
- grad_w_down: float32 [3072, 768], P(('heads', 'pages'))
- grad_rel_bias: float32 [3, 128, 12], P(None, 'pages', 'heads')
- grad_conv_w: float32 [18, 768], P(None, ('pages', 'heads'))
- grad_biases: float32 [6, 768], P(None, ('pages', 'heads'))
- grad_gains: float32 [2, 768], P(None, ('pages', 'heads'))
The draws below stay inside these ranges and needn't reach their ends.
Inputs may be any that keep to these rules, and one draw needn't show every extreme that they name: `text_len`: every page has at most 512 text tokens, and some page has exactly 512. `grid_index`: each page's row names every cell of the grid once.
All inputs are finite; a program needn't handle non-finite values.
Results may differ from the reference program's by a relative error of at most 0.024.
The reference program's roundings to bfloat16 on the way count: a program that leaves them out, or rounds other values in their place, can miss the bound.
Values may be sent and summed in bfloat16 or wider, within the bound.
A program may use at most 192 MiB of HBM per device.

```python
import jax
import jax.numpy as jnp
from jax import lax

D = 768
H = 12
HD = 64
FF = 3072
TXT = 512
GRID = 7
NB = 128
PAGES = 32
SEQ = 561
N_HEADS = 4


def draw_text_len(key, part):
    shortest = min(40, TXT // 2)
    lengths = jax.random.randint(key, (PAGES,), shortest, TXT + 1)
    chosen = jax.random.randint(jax.random.fold_in(key, 7), (), 0, PAGES)
    return jnp.where(jnp.arange(PAGES) == chosen, TXT, lengths).astype(jnp.int32)


def with_ends(values, stream_key, smallest, top_value):
    spot = [jax.random.randint(jax.random.fold_in(stream_key, axis), (), 0, length) for axis, length in enumerate(values.shape)]
    main_axis = values.shape.index(max(values.shape))
    beside = spot[:main_axis] + [(spot[main_axis] + 1) % values.shape[main_axis]] + spot[main_axis + 1:]
    return values.at[tuple(spot)].set(smallest).at[tuple(beside)].set(top_value)


def strengthened(array, stream_key, source, target, parts, factor):
    def block_of(position):
        return (jnp.arange(array.shape[position]) // (array.shape[position] // parts)).reshape((-1,) + (1,) * (array.ndim - 1 - position))

    near = jax.random.permutation(stream_key, parts)[block_of(target)]
    far = (block_of(target) + parts // 2) % parts
    return jnp.where((block_of(source) == near) | (block_of(source) == far), factor * array, array)


def steps_of(stream_key, shape, split, smallest, top_value):
    gain = 1.0
    for axis_at, blocks in split:
        steps = jax.random.uniform(jax.random.fold_in(jax.random.fold_in(stream_key, 6), axis_at), (blocks,), jnp.float32, smallest / len(split), top_value / len(split))
        gain = gain * jnp.repeat(jnp.exp(steps), shape[axis_at] // blocks).reshape((-1,) + (1,) * (len(shape) - 1 - axis_at))
    return gain


def scatter_about(key, dims, deviation, bound, split=(), kind=jnp.bfloat16):
    factor_of = steps_of(key, dims, split, -0.22, 0.18) if split else 1.0
    drawn = jax.random.normal(key, dims, jnp.float32) * deviation * factor_of
    return jnp.minimum(jnp.maximum(drawn, -bound), bound).astype(kind)


def noise_with(own_key, shape, deviation, most, shards, heavy, held_as=jnp.bfloat16):
    values = deviation * jax.random.normal(own_key, shape, jnp.float32)
    if shards:
        values = values * steps_of(own_key, shape, shards, -0.22, 0.18)
    return jnp.clip(strengthened(values, jax.random.fold_in(own_key, 3), *heavy), -most, most).astype(held_as)


def setup_inputs(seed: int = 0) -> dict:
    arg_keys = jax.random.split(jax.random.key(seed), 16)
    return {
        "x_in": noise_with(arg_keys[0], (PAGES, SEQ, D), 1.0, 6.0, ((0, 8),), (0, 2, 8, 2.0)),
        "cotangent": scatter_about(arg_keys[1], (PAGES, SEQ, D), 1.0, 6.0, ((0, 8),)),
        "text_len": draw_text_len(jax.random.fold_in(arg_keys[15], 71), 0),
        "coords": with_ends(jax.random.randint(arg_keys[3], (PAGES, 3, SEQ), 0, 2 * NB), jax.random.fold_in(arg_keys[3], 1), 0, (2 * NB) - 1).astype(jnp.int32),
        "grid_index": jax.vmap(lambda own: jax.random.permutation(own, GRID * GRID))(jax.random.split(arg_keys[4], PAGES)).reshape((PAGES, GRID * GRID)).astype(jnp.int32),
        "w_qkv": scatter_about(arg_keys[5], (D, 3, D), D ** -0.5, 0.21875, ((0, 8), (2, 4))),
        "b_qv": scatter_about(arg_keys[6], (2, D), 0.5, 3.0, ((1, 32),)),
        "w_out": scatter_about(arg_keys[7], (D, D), (D // 16) ** -0.5, 0.875, ((0, 32),)),
        "w_up": scatter_about(arg_keys[8], (D, FF), D ** -0.5, 0.21875, ((0, 8), (1, 4))),
        "b_up": scatter_about(arg_keys[9], (FF,), 0.5, 3.0, ((0, 32),)),
        "w_down": scatter_about(arg_keys[10], (FF, D), FF ** -0.5, 0.109375, ((0, 32),)),
        "rel_bias": scatter_about(arg_keys[11], (3, NB, H), 0.5, 3.0, ((1, 8), (2, 4))),
        "conv_w": scatter_about(arg_keys[12], (18, D), 0.3, 2.0, ((1, 32),)),
        "biases": scatter_about(arg_keys[13], (6, D), 0.3, 2.0, ((1, 32),)),
        "gains": jnp.clip(1.0 + 0.1 * jax.random.normal(arg_keys[14], (2, D), jnp.float32), 0.5, 1.5).astype(jnp.bfloat16),
    }


HIGHEST = lax.Precision.HIGHEST
EPSILON = 1e-05

@jax.custom_vjp
def low(v):
    return lax.optimization_barrier(v.astype(jnp.bfloat16)).astype(jnp.float32)

@jax.custom_vjp
def low_back(v):
    return v

def low_keep(v):
    return (low(v), None)

def low_pass(kept, grad):
    return (grad,)

def back_keep(v):
    return (v, None)

def back_low(kept, grad):
    return (low(grad),)
low.defvjp(low_keep, low_pass)
low_back.defvjp(back_keep, back_low)

def layer_norm(values, gain_row, shift_row):
    average = lax.optimization_barrier(jnp.mean(values, -1, keepdims=True))
    centred = values - average
    variance = lax.optimization_barrier(jnp.mean(centred * centred, -1, keepdims=True))
    return centred * lax.rsqrt(variance + EPSILON) * gain_row + shift_row

def valid_slots(text_len, seq_len):
    positions = jnp.arange(seq_len, dtype=jnp.int32)
    return jnp.logical_or(positions[None, :] < text_len[:, None], positions[None, :] >= TXT)

def bucket_ids(coords_page):
    offsets = coords_page[:, None, :] - coords_page[:, :, None]
    return (jnp.clip(offsets, -(NB // 2), NB // 2 - 1) + NB // 2).astype(jnp.int32)

def dcpe(field, valid, grid_index, kernel, first_bias, second_bias):
    page_count = field.shape[0]
    model_width = field.shape[-1]
    cell_count = GRID * GRID
    masked = field * valid[:, :, None].astype(field.dtype)
    text_part = masked[:, :TXT]
    padded = jnp.pad(text_part, ((0, 0), (3, 3), (0, 0)))
    text_out = jnp.zeros_like(text_part) + first_bias
    for spacing in range(1, 4):
        for offset_no in range(3):
            shift_at = 3 + (offset_no - 1) * spacing
            text_out = text_out + kernel[3 * (spacing - 1) + offset_no] * padded[:, shift_at:shift_at + TXT]
    placement = (grid_index[:, :, None] == jnp.arange(cell_count, dtype=jnp.int32)[None, None, :]).astype(field.dtype)
    on_grid = jnp.einsum('psc,psd->pcd', placement, masked[:, TXT:], precision=HIGHEST)
    on_grid = jnp.pad(on_grid.reshape(page_count, GRID, GRID, model_width), ((0, 0), (1, 1), (1, 1), (0, 0)))
    grid_out = jnp.zeros((page_count, GRID, GRID, model_width), field.dtype) + second_bias
    for row_no in range(3):
        for col_no in range(3):
            grid_out = grid_out + kernel[9 + 3 * row_no + col_no] * on_grid[:, row_no:row_no + GRID, col_no:col_no + GRID]
    patch_out = jnp.einsum('psc,pcd->psd', placement, grid_out.reshape(page_count, cell_count, model_width), precision=HIGHEST)
    return jnp.concatenate([text_out, patch_out], 1)

def attend(queries, key_rows, value_rows, valid_page, coords_page, rel_table):
    bucket = bucket_ids(coords_page)
    rel_terms = rel_table[0][bucket[0]] + rel_table[1][bucket[1]] + rel_table[2][bucket[2]]
    scores = jnp.einsum('ihd,jhd->hij', queries, key_rows, precision=HIGHEST) * 0.125 + jnp.transpose(rel_terms, (2, 0, 1))
    scores = low_back(scores)
    scores = jnp.where(valid_page[None, None, :], scores, -1e+30)
    highest = lax.optimization_barrier(jnp.max(scores, -1, keepdims=True))
    weights = jnp.exp(scores - highest)
    probs = low(weights / lax.optimization_barrier(jnp.sum(weights, -1, keepdims=True)))
    return jnp.einsum('hij,jhd->ihd', probs, value_rows, precision=HIGHEST)

def reference(x_in, cotangent, text_len, coords, grid_index, w_qkv, b_qv, w_out, w_up, b_up, w_down, rel_bias, conv_w, biases, gains):
    page_count, seq_len, model_width = x_in.shape
    valid = valid_slots(text_len, seq_len)
    group_width = model_width // N_HEADS
    group_hidden = FF // N_HEADS

    def forward(field, qkv_w, qv_b, out_w, up_w, up_b, down_w, rel_table, kernel, bias_rows, gain_rows):
        h_one = field + dcpe(field, valid, grid_index, kernel, bias_rows[0], bias_rows[1])
        act_in = low(h_one)
        queries = low_back(low(jnp.einsum('psd,de->pse', act_in, qkv_w[:, 0], precision=HIGHEST) + qv_b[0]))
        key_rows = low_back(low(jnp.einsum('psd,de->pse', act_in, qkv_w[:, 1], precision=HIGHEST)))
        value_rows = low_back(low(jnp.einsum('psd,de->pse', act_in, qkv_w[:, 2], precision=HIGHEST) + qv_b[1]))
        split_shape = (page_count, seq_len, H, HD)
        step_fn = jax.checkpoint(lambda entry: attend(entry[0], entry[1], entry[2], entry[3], entry[4], rel_table))
        mixed = lax.map(step_fn, (queries.reshape(split_shape), key_rows.reshape(split_shape), value_rows.reshape(split_shape), valid, coords))
        mixed = low_back(low(mixed.reshape(page_count, seq_len, model_width)))
        attn_sum = jnp.zeros_like(field)
        for group in range(N_HEADS):
            lower = group * group_width
            attn_sum = attn_sum + low(jnp.einsum('psc,cd->psd', mixed[:, :, lower:lower + group_width], out_w[lower:lower + group_width], precision=HIGHEST))
        attn = low_back(attn_sum + bias_rows[2])
        h_two = layer_norm(h_one + attn, gain_rows[0], bias_rows[3])
        ffn_in = low(h_two)
        hidden = low_back(jnp.einsum('psd,df->psf', ffn_in, up_w, precision=HIGHEST) + up_b)
        activated = low(jax.nn.gelu(hidden, approximate=False))
        ffn_sum = jnp.zeros_like(field)
        for group in range(N_HEADS):
            lower = group * group_hidden
            ffn_sum = ffn_sum + low(jnp.einsum('psf,fd->psd', activated[:, :, lower:lower + group_hidden], down_w[lower:lower + group_hidden], precision=HIGHEST))
        ffn = low_back(ffn_sum + bias_rows[4])
        return layer_norm(h_two + ffn, gain_rows[1], bias_rows[5])
    f32 = jnp.float32
    result, pullback = jax.vjp(forward, x_in.astype(f32), w_qkv.astype(f32), b_qv.astype(f32), w_out.astype(f32), w_up.astype(f32), b_up.astype(f32), w_down.astype(f32), rel_bias.astype(f32), conv_w.astype(f32), biases.astype(f32), gains.astype(f32))
    grads = pullback(cotangent.astype(f32))
    return (result.astype(jnp.bfloat16), grads[0], grads[1], grads[2], grads[3], grads[4], grads[5], grads[6], grads[7], grads[8], grads[9], grads[10])
```

```python
import functools

import jax
import jax.numpy as jnp
from jax import lax
from jax.experimental import pallas as pl
from jax.experimental.pallas import tpu as pltpu
from jax.sharding import PartitionSpec as P

HD = 64
TXT = 512
GRID = 7
NB = 128


HIGHEST = lax.Precision.HIGHEST
EPSILON = 1e-05


def layer_norm(values, gain_row, shift_row):
    average = jnp.mean(values, -1, keepdims=True)
    centred = values - average
    variance = jnp.mean(centred * centred, -1, keepdims=True)
    return centred * lax.rsqrt(variance + EPSILON) * gain_row + shift_row


def valid_slots(text_len, seq_len):
    positions = jnp.arange(seq_len, dtype=jnp.int32)
    return jnp.logical_or(positions[None, :] < text_len[:, None], positions[None, :] >= TXT)


def offset_table():
    span_ids = jnp.arange(2 * NB, dtype=jnp.int32)
    offsets = span_ids[None, :] - span_ids[:, None]
    bucket_of = jnp.clip(offsets, -(NB // 2), NB // 2 - 1) + NB // 2
    return (bucket_of[:, :, None] == jnp.arange(NB, dtype=jnp.int32)[None, None, :]).astype(
        jnp.bfloat16
    )


def placed_of(coords_page):
    return (coords_page[:, :, None] == jnp.arange(2 * NB, dtype=jnp.int32)[None, None, :]).astype(
        jnp.bfloat16
    )


def toeplitz_of(offsets_map, rel_table):
    return jnp.einsum(
        "abk,ckh->chab", offsets_map, rel_table, preferred_element_type=jnp.float32
    ).astype(jnp.bfloat16)


def dcpe(field, valid, grid_index, kernel, first_bias, second_bias):
    page_count = field.shape[0]
    model_width = field.shape[-1]
    cell_count = GRID * GRID
    masked = field * valid[:, :, None].astype(field.dtype)
    text_part = masked[:, :TXT]
    padded = jnp.pad(text_part, ((0, 0), (3, 3), (0, 0)))
    text_out = jnp.zeros_like(text_part) + first_bias
    for spacing in range(1, 4):
        for offset_no in range(3):
            shift_at = 3 + (offset_no - 1) * spacing
            text_out = (
                text_out
                + kernel[3 * (spacing - 1) + offset_no] * padded[:, shift_at : shift_at + TXT]
            )
    placement = (
        grid_index[:, :, None] == jnp.arange(cell_count, dtype=jnp.int32)[None, None, :]
    ).astype(field.dtype)
    on_grid = jnp.einsum("psc,psd->pcd", placement, masked[:, TXT:], precision=HIGHEST)
    on_grid = jnp.pad(
        on_grid.reshape(page_count, GRID, GRID, model_width), ((0, 0), (1, 1), (1, 1), (0, 0))
    )
    grid_out = jnp.zeros((page_count, GRID, GRID, model_width), field.dtype) + second_bias
    for row_no in range(3):
        for col_no in range(3):
            grid_out = (
                grid_out
                + kernel[9 + 3 * row_no + col_no]
                * on_grid[:, row_no : row_no + GRID, col_no : col_no + GRID]
            )
    patch_out = jnp.einsum(
        "psc,pcd->psd",
        placement,
        grid_out.reshape(page_count, cell_count, model_width),
        precision=HIGHEST,
    )
    return jnp.concatenate([text_out, patch_out], 1)


def page_scores(queries, key_rows, valid_page, placed, toeplitz):
    products = (
        jnp.einsum("ihd,jhd->hij", queries, key_rows, preferred_element_type=jnp.float32) * 0.125
    )
    left_part = jnp.einsum(
        "cia,chab->chib", placed, toeplitz, preferred_element_type=jnp.float32
    ).astype(jnp.bfloat16)
    rel_terms = jnp.einsum("chib,cjb->hij", left_part, placed, preferred_element_type=jnp.float32)
    return jnp.where(valid_page[None, None, :], products + rel_terms, -1e30)


def attend_page(queries, key_rows, value_rows, valid_page, coords_page, toeplitz):
    scores = page_scores(queries, key_rows, valid_page, placed_of(coords_page), toeplitz)
    highest = jnp.max(scores, -1, keepdims=True)
    weights = jnp.exp(scores - highest)
    norm_total = jnp.sum(weights, -1, keepdims=True)
    probs = (weights / norm_total).astype(jnp.bfloat16)
    mixed = jnp.einsum(
        "hij,jhd->ihd", probs, value_rows, preferred_element_type=jnp.float32
    ).astype(jnp.bfloat16)
    return (mixed, (highest + jnp.log(norm_total))[..., 0])


def back_page(queries, key_rows, value_rows, valid_page, coords_page, toeplitz, log_total, d_mixed):
    placed = placed_of(coords_page)
    scores = page_scores(queries, key_rows, valid_page, placed, toeplitz)
    probs = jnp.exp(scores - log_total[..., None])
    d_probs = jnp.einsum("ihd,jhd->hij", d_mixed, value_rows, preferred_element_type=jnp.float32)
    centre = jnp.sum(probs * d_probs, -1, keepdims=True)
    d_scores = (probs * (d_probs - centre)).astype(jnp.bfloat16)
    d_query = (
        jnp.einsum("hij,jhd->ihd", d_scores, key_rows, preferred_element_type=jnp.float32) * 0.125
    ).astype(jnp.bfloat16)
    d_key = (
        jnp.einsum("hij,ihd->jhd", d_scores, queries, preferred_element_type=jnp.float32) * 0.125
    ).astype(jnp.bfloat16)
    d_value = jnp.einsum(
        "hij,ihd->jhd", probs.astype(jnp.bfloat16), d_mixed, preferred_element_type=jnp.float32
    ).astype(jnp.bfloat16)
    spread = jnp.einsum("cia,hij->chaj", placed, d_scores, preferred_element_type=jnp.float32)
    table_grad = jnp.einsum("chaj,cjb->chab", spread, placed.astype(jnp.float32), precision=HIGHEST)
    return (d_query, d_key, d_value, table_grad)


MESH = pl.DeviceIdType.MESH


def place():
    p, h = lax.axis_index("pages"), lax.axis_index("heads")
    return p, h, p // 2, p % 2, h // 2, h % 2


def greet(devices, count):
    barrier = pltpu.get_barrier_semaphore()
    for device in devices:
        pl.semaphore_signal(barrier, inc=1, device_id=device, device_id_type=MESH)
    pl.semaphore_wait(barrier, count)


def neighbours(p, h, z, y, x, c, n_z):
    core = (p, 2 * x + 1 - c)
    across = (p, 2 * (1 - x) + c)
    beside = (2 * z + 1 - y, h)
    line = [(2 * lax.rem(z + dz, n_z) + y, h) for dz in range(1, n_z)]
    return core, across, beside, line


def gather_kernel(n_p, late, early, *refs):
    n = len(late) + len(early)
    srcs, dsts = refs[:n], refs[n : 2 * n]
    send_sem, recv_sem, local_sem = refs[2 * n :]
    n_z = n_p // 2
    p, h, z, y, x, c = place()
    core, across, beside, line = neighbours(p, h, z, y, x, c, n_z)
    greet([core, across, beside] + line, 3 + len(line))
    h_x = 2 * (1 - x) + c

    n_line = n_z - 1
    started = []

    def copy(k, src, bh, bp, device, slot):
        return pltpu.make_async_remote_copy(
            src_ref=src,
            dst_ref=dsts[k].at[bh, bp],
            send_sem=send_sem.at[k, slot],
            recv_sem=recv_sem.at[k, bh, bp],
            device_id=device,
            device_id_type=MESH,
        )

    used = [0] * n

    def send(k, bh, bp, device, own=False):
        src = srcs[k] if own else dsts[k].at[bh, bp]
        item = copy(k, src, bh, bp, device, used[k])
        used[k] += 1
        item.start()
        started.append(item)

    def arrived(k, bh, bp):
        copy(k, dsts[k].at[bh, bp], bh, bp, core, 0).wait_recv()

    for k in early:
        send(k, h, p, across, own=True)
    for device in line:
        for k in late:
            send(k, h, p, device, own=True)
    for k in late:
        send(k, h, p, beside, own=True)
        send(k, h, p, across, own=True)
    for device in line:
        for k in early:
            send(k, h, p, device, own=True)
    for k in early:
        send(k, h, p, beside, own=True)
    for k in late + early:
        send(k, h, p, core, own=True)
    locals_ = []
    for k in range(n):
        item = pltpu.make_async_copy(srcs[k], dsts[k].at[h, p], local_sem.at[k])
        item.start()
        locals_.append(item)
    for k in early:
        arrived(k, h_x, p)
        for device in line:
            send(k, h_x, p, device)
        send(k, h_x, p, beside)
        send(k, h_x, p, core)
    for dz in range(1, n_z):
        q = 2 * lax.rem(z + n_z - dz, n_z) + y
        for k in late:
            arrived(k, h, q)
            send(k, h, q, beside)
            send(k, h, q, across)
            send(k, h, q, core)
        for k in early:
            for bh in (h, h_x):
                arrived(k, bh, q)
                send(k, bh, q, beside)
                send(k, bh, q, core)
    for dz in range(n_z):
        q = 2 * lax.rem(z + n_z - dz, n_z) + 1 - y
        for k in late:
            arrived(k, h, q)
            send(k, h, q, across)
            send(k, h, q, core)
        for k in early:
            for bh in (h, h_x):
                arrived(k, bh, q)
                send(k, bh, q, core)
    for k in late:
        for dz in range(n_z):
            for side in (y, 1 - y):
                q = 2 * lax.rem(z + n_z - dz, n_z) + side
                arrived(k, h_x, q)
                send(k, h_x, q, core)
    for k in late + early:
        for bx in (x, 1 - x):
            for dz in range(n_z):
                for side in (y, 1 - y):
                    q = 2 * lax.rem(z + n_z - dz, n_z) + side
                    arrived(k, 2 * bx + 1 - c, q)
    for item in locals_:
        item.wait()
    for item in started:
        item.wait_send()


def gather_all(shards, n_h, n_p, late, early):
    outs = [jax.ShapeDtypeStruct((n_h, n_p) + s.shape, s.dtype) for s in shards]
    n = len(shards)
    total = n_h * n_p
    if n_h != 4 or total > 32:
        return [
            lax.all_gather(lax.all_gather(s, "pages", axis=0), "heads", axis=0) for s in shards
        ]
    return pl.pallas_call(
        functools.partial(gather_kernel, n_p, late, early),
        name="gather_weights",
        out_shape=outs,
        in_specs=[pl.BlockSpec(memory_space=pltpu.VMEM)] * n,
        out_specs=[pl.BlockSpec(memory_space=pl.ANY)] * n,
        scratch_shapes=[
            pltpu.SemaphoreType.DMA((n, total)),
            pltpu.SemaphoreType.DMA((n, n_h, n_p)),
            pltpu.SemaphoreType.DMA((n,)),
        ],
        compiler_params=pltpu.CompilerParams(collective_id=0, has_side_effects=True),
    )(*shards)


def reduce_kernel(n_p, late, early, *refs):
    n = len(late) + len(early)
    srcs, dsts = refs[:n], refs[n : 2 * n]
    boxes = refs[2 * n : 6 * n]
    r1, r2, r3, r4 = boxes[:n], boxes[n : 2 * n], boxes[2 * n : 3 * n], boxes[3 * n :]
    send_sem, recv_sem = refs[6 * n :]
    n_z = n_p // 2
    p, h, z, y, x, c = place()
    core, across, beside, line = neighbours(p, h, z, y, x, c, n_z)
    greet([core, across, beside] + line, 3 + len(line))
    f32 = jnp.float32
    at2, at3, at4 = 2 * n_p, 4 * n_p, 6 * n_p

    def copy(k, src, dst, slot, device, out_slot=None):
        return pltpu.make_async_remote_copy(
            src_ref=src,
            dst_ref=dst,
            send_sem=send_sem.at[k, slot if out_slot is None else out_slot],
            recv_sem=recv_sem.at[k, slot],
            device_id=device,
            device_id_type=MESH,
        )

    def page_of(i):
        return 2 * lax.rem(z + lax.div(i, 2) + 1, n_z) + lax.rem(1 - y + i, 2)

    def core_copy(k, xh, q):
        return copy(k, srcs[k].at[2 * xh + 1 - c, q], r1[k].at[xh, q], xh * n_p + q, core)

    def x_copy(k, q):
        return copy(k, r1[k].at[1 - x, q], r2[k].at[q], at2 + q, across)

    def y_copy(k, zq):
        return copy(k, r1[k].at[x, 2 * zq + 1 - y], r3[k].at[zq], at3 + zq, beside)

    def z_copy(k, zq, device):
        return copy(k, r1[k].at[x, 2 * zq + y], r4[k].at[z], at4 + z, device, at4 + zq)

    def z_wait(k, zq):
        return copy(k, r4[k].at[zq], r4[k].at[zq], at4 + zq, core)

    def y2_copy(k, xh, zq):
        return copy(k, r1[k].at[xh, 2 * zq + 1 - y], r2[k].at[xh, zq], at2 + xh * n_z + zq, beside)

    def z2_copy(k, xh, zq, device):
        src = r1[k].at[xh, 2 * zq + y]
        return copy(k, src, r3[k].at[xh, z], at3 + xh * n_z + z, device, at3 + xh * n_z + zq)

    def z2_wait(k, xh, zq):
        return copy(k, r3[k].at[xh, zq], r3[k].at[xh, zq], at3 + xh * n_z + zq, core)

    def x2_copy(k):
        return copy(k, r1[k].at[1 - x, 2 * z + y], r4[k].at[0], at4, across)

    def each(count, body):
        lax.fori_loop(0, count, lambda i, carry: (body(i), carry)[1], jnp.int32(0))

    def begin_late(i):
        for k in late:
            core_copy(k, 1 - x, page_of(i)).start()

    def begin_early(i):
        for xh in (1 - x, x):
            for k in early:
                core_copy(k, xh, 2 * lax.rem(z + i + 1, n_z) + y).start()

    def begin_early_y(i):
        for xh in (1 - x, x):
            for k in early:
                core_copy(k, xh, 2 * lax.rem(z + i + 1, n_z) + 1 - y).start()

    def begin_rest(i):
        for k in late:
            core_copy(k, x, page_of(i)).start()

    each(n_p, begin_late)
    each(n_z, begin_early_y)
    each(n_p, begin_rest)
    each(n_z, begin_early)

    def x_stage(i):
        q = page_of(i)
        for k in late:
            core_copy(k, 1 - x, q).wait_recv()
            total = srcs[k][2 * (1 - x) + c, q].astype(f32) + r1[k][1 - x, q].astype(f32)
            r1[k][1 - x, q] = total.astype(r1[k].dtype)
        for k in late:
            x_copy(k, q).start()

    def early_y_stage(i):
        zq = lax.rem(z + i + 1, n_z)
        q = 2 * zq + 1 - y
        for k in early:
            for xh in (1 - x, x):
                core_copy(k, xh, q).wait_recv()
                total = srcs[k][2 * xh + c, q].astype(f32) + r1[k][xh, q].astype(f32)
                r1[k][xh, q] = total.astype(r1[k].dtype)
        for k in early:
            for xh in (1 - x, x):
                y2_copy(k, xh, zq).start()

    def both(i):
        x_stage(2 * i)
        x_stage(2 * i + 1)
        early_y_stage(i)

    each(n_z, both)

    def early_z_stage(i):
        zq = lax.rem(z + i + 1, n_z)
        q = 2 * zq + y
        for k in early:
            for xh in (1 - x, x):
                core_copy(k, xh, q).wait_recv()
                y2_copy(k, xh, zq).wait_recv()
                total = srcs[k][2 * xh + c, q].astype(f32) + r1[k][xh, q].astype(f32)
                total = total + r2[k][xh, zq].astype(f32)
                r1[k][xh, q] = total.astype(r1[k].dtype)
        return zq

    def late_y_stage(i):
        zq = lax.rem(z + i + 1, n_z)
        q = 2 * zq + 1 - y
        for k in late:
            core_copy(k, x, q).wait_recv()
            x_copy(k, q).wait_recv()
            total = srcs[k][h, q].astype(f32) + r1[k][x, q].astype(f32) + r2[k][q].astype(f32)
            r1[k][x, q] = total.astype(r1[k].dtype)
        for k in late:
            y_copy(k, zq).start()

    def late_z_stage(i):
        zq = lax.rem(z + i + 1, n_z)
        q = 2 * zq + y
        for k in late:
            core_copy(k, x, q).wait_recv()
            x_copy(k, q).wait_recv()
            y_copy(k, zq).wait_recv()
            total = srcs[k][h, q].astype(f32) + r1[k][x, q].astype(f32)
            total = total + r2[k][q].astype(f32) + r3[k][zq].astype(f32)
            r1[k][x, q] = total.astype(r1[k].dtype)
        return zq

    def early_line(i):
        zq = early_z_stage(i)
        for k in early:
            for xh in (1 - x, x):
                z2_copy(k, xh, zq, (2 * zq + y, h)).start()

    def late_line(i):
        zq = late_z_stage(i)
        for k in late:
            z_copy(k, zq, (2 * zq + y, h)).start()

    def stage_two(i):
        late_y_stage(i)

    each(n_z, stage_two)
    each(n_z - 1, early_line)
    each(n_z - 1, late_line)

    mine = 2 * z + y
    for k in early:
        for xh in (1 - x, x):
            core_copy(k, xh, mine).wait_recv()
            y2_copy(k, xh, z).wait_recv()
        total = srcs[k][2 * (1 - x) + c, mine].astype(f32) + r1[k][1 - x, mine].astype(f32)
        total = total + r2[k][1 - x, z].astype(f32)
        for dz in range(1, n_z):
            zq = lax.rem(z + n_z - dz, n_z)
            z2_wait(k, 1 - x, zq).wait_recv()
            total = total + r3[k][1 - x, zq].astype(f32)
        r1[k][1 - x, mine] = total.astype(r1[k].dtype)
        x2_copy(k).start()
    for k in late:
        core_copy(k, x, mine).wait_recv()
        x_copy(k, mine).wait_recv()
        y_copy(k, z).wait_recv()
        total = srcs[k][h, mine].astype(f32) + r1[k][x, mine].astype(f32)
        total = total + r2[k][mine].astype(f32) + r3[k][z].astype(f32)
        for dz in range(1, n_z):
            zq = lax.rem(z + n_z - dz, n_z)
            z_wait(k, zq).wait_recv()
            total = total + r4[k][zq].astype(f32)
        dsts[k][...] = total
    for k in early:
        total = srcs[k][h, mine].astype(f32) + r1[k][x, mine].astype(f32) + r2[k][x, z].astype(f32)
        for dz in range(1, n_z):
            zq = lax.rem(z + n_z - dz, n_z)
            z2_wait(k, x, zq).wait_recv()
            total = total + r3[k][x, zq].astype(f32)
        x2_copy(k).wait_recv()
        dsts[k][...] = total + r4[k][0].astype(f32)

    def sent_pages(q):
        for k in range(n):
            for xh in (0, 1):
                core_copy(k, xh, q).wait_send()
        for k in late:
            x_copy(k, q).wait_send()

    def sent_lines(zq):
        for k in late:
            y_copy(k, zq).wait_send()
        for k in early:
            for xh in (0, 1):
                y2_copy(k, xh, zq).wait_send()

    each(n_p, sent_pages)
    each(n_z, sent_lines)
    for k in early:
        x2_copy(k).wait_send()

    def sent_peer(i):
        zq = lax.rem(z + i + 1, n_z)
        for k in late:
            z_copy(k, zq, core).wait_send()
        for k in early:
            for xh in (0, 1):
                z2_copy(k, xh, zq, core).wait_send()

    each(n_z - 1, sent_peer)


def reduce_all(grads, n_h, n_p, late, early):
    outs = [jax.ShapeDtypeStruct(g.shape[2:], jnp.float32) for g in grads]
    n = len(grads)
    n_z = n_p // 2
    if n_h != 4 or n_h * n_p > 32:
        parts = [lax.psum_scatter(g.astype(jnp.float32), "heads", scatter_dimension=0) for g in grads]
        return [lax.psum_scatter(g, "pages", scatter_dimension=0) for g in parts]
    boxes = [[], [], [], []]
    for k, g in enumerate(grads):
        tail = g.shape[2:]
        leads = [(2, n_p), (n_p,), (n_z,), (n_z,)]
        if k in early:
            leads = [(2, n_p), (2, n_z), (2, n_z), (1,)]
        for box, lead in zip(boxes, leads):
            box.append(pltpu.VMEM(lead + tail, g.dtype))
    return pl.pallas_call(
        functools.partial(reduce_kernel, n_p, late, early),
        name="reduce_grads",
        out_shape=outs,
        in_specs=[pl.BlockSpec(memory_space=pltpu.VMEM)] * n,
        out_specs=[pl.BlockSpec(memory_space=pltpu.VMEM)] * n,
        scratch_shapes=sum(boxes, [])
        + [
            pltpu.SemaphoreType.DMA((n, 7 * n_p)),
            pltpu.SemaphoreType.DMA((n, 7 * n_p)),
        ],
        compiler_params=pltpu.CompilerParams(collective_id=1, has_side_effects=True),
    )(*grads)


def share_kernel(n, *refs):
    srcs, dsts = refs[:n], refs[n : 2 * n]
    send_sem, recv_sem, local_sem = refs[2 * n :]
    p, h = lax.axis_index("pages"), lax.axis_index("heads")
    x, c = h // 2, h % 2
    core, across = (p, 2 * x + 1 - c), (p, 2 * (1 - x) + c)
    greet([core, across], 2)
    h_x = 2 * (1 - x) + c

    def copy(k, src, bh, device, slot):
        return pltpu.make_async_remote_copy(
            src_ref=src,
            dst_ref=dsts[k].at[bh],
            send_sem=send_sem.at[k, slot],
            recv_sem=recv_sem.at[k, bh],
            device_id=device,
            device_id_type=MESH,
        )

    started = []
    for k in range(n):
        item = copy(k, srcs[k], h, across, 0)
        item.start()
        started.append(item)
    for k in range(n):
        item = copy(k, srcs[k], h, core, 1)
        item.start()
        started.append(item)
    own = []
    for k in range(n):
        item = pltpu.make_async_copy(srcs[k], dsts[k].at[h], local_sem.at[k])
        item.start()
        own.append(item)
    for k in range(n):
        copy(k, dsts[k].at[h_x], h_x, core, 0).wait_recv()
        item = copy(k, dsts[k].at[h_x], h_x, core, 2)
        item.start()
        started.append(item)
    for k in range(n):
        for bx in (x, 1 - x):
            bh = 2 * bx + 1 - c
            copy(k, dsts[k].at[bh], bh, core, 0).wait_recv()
    for item in own:
        item.wait()
    for item in started:
        item.wait_send()


def share_pages(pages, n_h):
    n = len(pages)
    if n_h != 4:
        return [lax.all_gather(page, "heads", axis=0) for page in pages]
    return pl.pallas_call(
        functools.partial(share_kernel, n),
        name="share_pages",
        out_shape=[jax.ShapeDtypeStruct((n_h,) + page.shape, page.dtype) for page in pages],
        in_specs=[pl.BlockSpec(memory_space=pltpu.VMEM)] * n,
        out_specs=[pl.BlockSpec(memory_space=pl.ANY)] * n,
        scratch_shapes=[
            pltpu.SemaphoreType.DMA((n, 3)),
            pltpu.SemaphoreType.DMA((n, n_h)),
            pltpu.SemaphoreType.DMA((n,)),
        ],
        compiler_params=pltpu.CompilerParams(collective_id=2, has_side_effects=True),
    )(*pages)


def pack_small(conv_w, biases, gains, b_qv, b_up, rel_bias):
    flat = jnp.concatenate(
        [v.reshape(-1) for v in (conv_w, biases, gains, b_qv, b_up, rel_bias)]
    )
    room = -flat.shape[0] % 1024
    return jnp.pad(flat, (0, room)).reshape(-1, 128)


def unpack_small(blocks, sizes):
    n_h, n_p = blocks.shape[:2]
    flat = blocks.reshape(n_h, n_p, -1)
    parts, at = [], 0
    for shape in sizes:
        count = 1
        for extent in shape:
            count *= extent
        parts.append(flat[:, :, at : at + count].reshape((n_h, n_p) + shape))
        at += count
    return parts


def local(
    x_in,
    cotangent,
    text_len,
    coords,
    grid_index,
    w_qkv,
    b_qv,
    w_out,
    w_up,
    b_up,
    w_down,
    rel_bias,
    conv_w,
    biases,
    gains,
    n_h,
    n_p,
):
    f32 = jnp.float32
    bf16 = jnp.bfloat16
    head_id = lax.axis_index("heads")
    seq_len, model_width = x_in.shape[1:]
    part = w_qkv.shape[2]
    heads_here = part // HD
    n_heads = heads_here * n_h
    rows_in = w_qkv.shape[0]
    small_sizes = [v.shape for v in (conv_w, biases, gains, b_qv, b_up, rel_bias)]
    late, early = [0, 1, 2, 3], [4]
    gathered = gather_all(
        [
            pack_small(conv_w, biases, gains, b_qv, b_up, rel_bias),
            w_qkv.reshape(rows_in, 3 * part),
            w_out,
            w_up,
            w_down,
        ],
        n_h,
        n_p,
        late,
        early,
    )
    conv_s, bias_s, gain_s, bqv_s, bup_s, rel_s = unpack_small(gathered[0], small_sizes)

    def columns(blocks):
        return jnp.transpose(blocks, (2, 1, 0, 3)).reshape(blocks.shape[2], -1)

    kernel_float = columns(conv_s).astype(f32)
    bias_float = columns(bias_s).astype(f32)
    gain_float = columns(gain_s).astype(f32)
    bqv_full = jnp.transpose(bqv_s, (2, 0, 1, 3)).reshape(2, n_h, part).astype(f32)
    bup_full = bup_s.reshape(-1).astype(f32)
    rel_full = jnp.transpose(rel_s, (2, 1, 3, 0, 4)).reshape(3, NB, n_heads)
    qkv_full = gathered[1].reshape(n_h, model_width, 3 * part)
    out_full = gathered[2].reshape(n_h, part, model_width)
    up_full = gathered[3].reshape(n_h, model_width, -1)
    down_full = gathered[4].reshape(n_h, up_full.shape[2], model_width)

    def mine(values):
        return lax.dynamic_index_in_dim(values, head_id, 0, keepdims=True)

    x_page, cot_page = mine(x_in), mine(cotangent)
    len_page, coords_page, grid_page = mine(text_len), mine(coords)[0], mine(grid_index)
    offsets_map = offset_table()
    toeplitz = toeplitz_of(offsets_map, rel_full)
    valid = valid_slots(len_page, seq_len)

    def conv_part(values, kernel, first_bias, second_bias):
        return dcpe(values, valid, grid_page, kernel, first_bias, second_bias)

    field = x_page.astype(f32)
    h_one = (field + conv_part(field, kernel_float, bias_float[0], bias_float[1]))[0]
    act_in = h_one.astype(bf16)
    qkv_bias = jnp.concatenate([bqv_full[0], jnp.zeros_like(bqv_full[0]), bqv_full[1]], -1)
    projected = (
        jnp.einsum("nd,hde->hne", act_in, qkv_full, preferred_element_type=f32)
        + qkv_bias[:, None, :]
    ).astype(bf16)

    def split(values):
        values = values.reshape(n_h, seq_len, heads_here, HD)
        return jnp.transpose(values, (1, 0, 2, 3)).reshape(seq_len, n_heads, HD)

    queries = split(projected[:, :, :part])
    key_rows = split(projected[:, :, part : 2 * part])
    value_rows = split(projected[:, :, 2 * part :])
    heads_out, log_total = attend_page(
        queries, key_rows, value_rows, valid[0], coords_page, toeplitz
    )
    mixed = heads_out.reshape(seq_len, n_h, part)
    attn = (
        jnp.sum(
            jnp.einsum("nhc,hcd->hnd", mixed, out_full, preferred_element_type=f32)
            .astype(bf16)
            .astype(f32),
            0,
        )
        + bias_float[2]
    )
    h_two_pre = h_one + attn
    h_two = layer_norm(h_two_pre, gain_float[0], bias_float[3])
    ffn_in = h_two.astype(bf16)
    bup_groups = bup_full.reshape(n_h, 1, -1)
    hidden = jnp.einsum("nd,hdf->hnf", ffn_in, up_full, preferred_element_type=f32) + bup_groups
    activated = jax.nn.gelu(hidden, approximate=False).astype(bf16)
    ffn = (
        jnp.sum(
            jnp.einsum("hnf,hfd->hnd", activated, down_full, preferred_element_type=f32)
            .astype(bf16)
            .astype(f32),
            0,
        )
        + bias_float[4]
    )
    summed = h_two + ffn
    result = layer_norm(summed, gain_float[1], bias_float[5])

    d_result = cot_page[0].astype(f32)
    norm_two_back = jax.vjp(layer_norm, summed, gain_float[1], bias_float[5])[1]
    d_sum, d_gain_two, d_shift_two = norm_two_back(d_result)
    d_ffn = d_sum.astype(bf16)
    grad_bias_down = jnp.sum(d_ffn.astype(f32), 0)
    grad_down = jnp.einsum("hnf,nd->hfd", activated, d_ffn, preferred_element_type=f32)
    d_act = jnp.einsum("nd,hfd->hnf", d_ffn, down_full, preferred_element_type=f32)
    gelu_back = jax.vjp(lambda inner: jax.nn.gelu(inner, approximate=False), hidden)[1]
    d_hidden = gelu_back(d_act)[0].astype(bf16)
    grad_up_bias = jnp.sum(d_hidden.astype(f32), 1)
    grad_up = jnp.einsum("nd,hnf->hdf", ffn_in, d_hidden, preferred_element_type=f32)
    d_two = d_sum + jnp.einsum("hnf,hdf->nd", d_hidden, up_full, preferred_element_type=f32)
    norm_one_back = jax.vjp(layer_norm, h_two_pre, gain_float[0], bias_float[3])[1]
    d_pre, d_gain_one, d_shift_one = norm_one_back(d_two)
    d_attn = d_pre.astype(bf16)
    grad_out_bias = jnp.sum(d_attn.astype(f32), 0)
    grad_out = jnp.einsum("nhc,nd->hcd", mixed, d_attn, preferred_element_type=f32)
    d_mixed = jnp.einsum("nd,hcd->nhc", d_attn, out_full, preferred_element_type=f32).astype(bf16)
    d_query, d_key, d_value, table_grad = back_page(
        queries,
        key_rows,
        value_rows,
        valid[0],
        coords_page,
        toeplitz,
        log_total,
        d_mixed.reshape(seq_len, n_heads, HD),
    )
    grad_rel = jnp.einsum("abk,chab->ckh", offsets_map.astype(f32), table_grad, precision=HIGHEST)

    def join(values):
        return jnp.transpose(values.reshape(seq_len, n_h, part), (1, 0, 2))

    d_proj = jnp.concatenate([join(d_query), join(d_key), join(d_value)], -1)
    grad_qkv = jnp.einsum("nd,hne->hde", act_in, d_proj, preferred_element_type=f32)
    row_sums = jnp.sum(d_proj.astype(f32), 1)
    grad_qv_bias = jnp.stack([row_sums[:, :part], row_sums[:, 2 * part :]])
    d_one = d_pre + jnp.einsum("hne,hde->nd", d_proj, qkv_full, preferred_element_type=f32)
    conv_back = jax.vjp(conv_part, field, kernel_float, bias_float[0], bias_float[1])[1]
    d_field, grad_kernel, d_first, d_second = conv_back(d_one[None])
    grad_x = d_one + d_field[0]
    grad_bias_rows = jnp.stack(
        [d_first, d_second, grad_out_bias, d_shift_one, grad_bias_down, d_shift_two]
    )
    grad_gain_rows = jnp.stack([d_gain_one, d_gain_two])

    def uncolumns(values):
        rows = values.shape[0]
        return jnp.transpose(values.reshape(rows, n_p, n_h, -1), (2, 1, 0, 3)).reshape(n_h, n_p, -1)

    flat = jnp.concatenate(
        [
            uncolumns(grad_kernel),
            uncolumns(grad_bias_rows),
            uncolumns(grad_gain_rows),
            jnp.transpose(grad_qv_bias.reshape(2, n_h, n_p, -1), (1, 2, 0, 3)).reshape(n_h, n_p, -1),
            grad_up_bias.reshape(n_h, n_p, -1),
            jnp.transpose(
                grad_rel.reshape(3, n_p, -1, n_h, heads_here), (3, 1, 0, 2, 4)
            ).reshape(n_h, n_p, -1),
        ],
        -1,
    )
    width = flat.shape[2]
    flat = jnp.pad(flat, ((0, 0), (0, 0), (0, -width % 1024))).reshape(n_h, n_p, -1, 128)

    def blocks(values):
        return values.reshape((n_h, n_p, -1) + values.shape[2:]).astype(bf16)

    reduced = reduce_all(
        [flat, blocks(grad_qkv), blocks(grad_out), blocks(grad_up), blocks(grad_down)],
        n_h,
        n_p,
        late,
        early,
    )
    small = unpack_small(reduced[0][None, None], small_sizes)
    small = [value[0, 0] for value in small]
    out_all, grad_x_all = share_pages([result.astype(bf16), grad_x.astype(bf16)], n_h)
    return (
        out_all,
        grad_x_all.astype(f32),
        reduced[1].reshape(rows_in, 3, part),
        small[3],
        reduced[2],
        reduced[3],
        small[4],
        reduced[4],
        small[5],
        small[0],
        small[1],
        small[2],
    )


def solution(mesh):
    n_h, n_p = mesh.shape["heads"], mesh.shape["pages"]
    return jax.shard_map(
        functools.partial(local, n_h=n_h, n_p=n_p),
        mesh=mesh,
        in_specs=(
            P("pages", None, None),
            P("pages", None, None),
            P("pages"),
            P("pages", None, None),
            P("pages", None),
            P("pages", None, "heads"),
            P(None, ("heads", "pages")),
            P(("heads", "pages"), None),
            P("pages", "heads"),
            P(("heads", "pages")),
            P(("heads", "pages"), None),
            P(None, "pages", "heads"),
            P(None, ("pages", "heads")),
            P(None, ("pages", "heads")),
            P(None, ("pages", "heads")),
        ),
        out_specs=(
            P("pages", None, None),
            P("pages", None, None),
            P("pages", None, "heads"),
            P(None, ("heads", "pages")),
            P(("heads", "pages"), None),
            P("pages", "heads"),
            P(("heads", "pages")),
            P(("heads", "pages"), None),
            P(None, "pages", "heads"),
            P(None, ("pages", "heads")),
            P(None, ("pages", "heads")),
            P(None, ("pages", "heads")),
        ),
        check_vma=False,
    )
```
